32 devices in a mesh: rep: 2 (over x), exp: 16 (over z, y, core).
Axes of the slice: x: 2, y: 2, z: 4, core: 2. Of those that a mesh axis runs over, the one named last changes fastest.
Arguments:
- a_tokens: bfloat16 [64, 7168], P(('rep', 'exp')), parts along dimension 0, may hold values from -6 to 6
- a_gain: float32 [7168], replicated, may hold values from 0.25 to 1.75
- dense_gate: bfloat16 [7168, 18432], P(None, 'exp'), may hold values from -0.0625 to 0.0625
- dense_up: bfloat16 [7168, 18432], P(None, 'exp'), may hold values from -0.0625 to 0.0625
- dense_down: bfloat16 [18432, 7168], P('exp'), may hold values from -0.046875 to 0.046875
- b_tokens: bfloat16 [128, 7168], P(('rep', 'exp')), parts along dimension 0, may hold values from -6 to 6
- b_gain: float32 [7168], replicated, may hold values from 0.25 to 1.75
- expert_ids: int32 [128, 8], P(('rep', 'exp')), parts along dimension 0, may hold values from 0 to 15, all different within a row; in each aligned block of 4 rows (0 to 3, 4 to 7, ...) at most 3 rows name the same one
- route_weights: float32 [128, 8], P(('rep', 'exp')), parts along dimension 0, may hold values from 0.05 to 0.5
- expert_gate: bfloat16 [16, 7168, 1024], P('exp'), may hold values from -0.0625 to 0.0625
- expert_up: bfloat16 [16, 7168, 1024], P('exp'), may hold values from -0.0625 to 0.0625
- expert_down: bfloat16 [16, 1024, 7168], P('exp'), may hold values from -0.1875 to 0.1875
Outputs:
- a_out: bfloat16 [64, 7168], P(('rep', 'exp')), parts along dimension 0
- b_out: bfloat16 [128, 7168], P(('rep', 'exp')), parts along dimension 0
The draws below stay inside these ranges and needn't reach their ends.
There are 2 independent parts, one for each index of `rep`. The reference program is written for one: setup_inputs(seed, part) draws one part's arguments, and reference() takes and returns one part's arrays. A program takes and returns all parts, laid end to end along the dimension named above; an argument that names none is the same for every part. Nothing has to cross between parts.
Inputs may be any that keep to these rules, and one draw needn't show every extreme that they name: `expert_ids`: each row names 8 different experts. Among the rows of one device no expert is named more than 3 times, and in some devices one expert is named exactly 3 times.
All inputs are finite; a program needn't handle non-finite values.
Results may differ from the reference program's by a relative error of at most 0.008.
Values may be sent and summed in bfloat16 or wider, within the bound.
A program may use at most 192 MiB of HBM per device.

```python
import math
import jax
import jax.numpy as jnp
import numpy as np
from jax import lax

D = 7168
FF = 18432
EH = 1024
EXPERTS = 16
TOPK = 8
TB_DEV = 4
TA = 32
TB = 64
GROUP = 1
ES = 1024
CAP = 3


def levels(stream_key, extent, pieces, low, high):
    def one(position, parts):
        draws = jax.random.uniform(jax.random.fold_in(jax.random.fold_in(stream_key, 6), position), (parts,), jnp.float32, low / len(pieces), high / len(pieces))
        return jnp.repeat(jnp.exp(draws), extent[position] // parts).reshape((-1,) + (1,) * (len(extent) - position - 1))

    level = one(*pieces[0])
    for cut in pieces[1:]:
        level = level * one(*cut)
    return level


def shared_out(stream_key, own, number, rows, amount, top, bound, slope):
    order = jax.random.permutation(stream_key, amount)
    packed, ordinary = load_shares(amount, rows * top, bound, slope, True), load_shares(amount, rows * top, bound, slope, False)
    places = jnp.arange(amount)

    def named(sizes, offset_by):
        used = int((sizes > 0).sum())
        fixed = max(1, used // 4)
        shifted = fixed + (places - fixed + offset_by * (used - fixed)) % max(1, amount - fixed)
        return jnp.zeros((amount,), jnp.int32).at[order[jnp.where(places < fixed, places, shifted)]].set(jnp.asarray(sizes, jnp.int32))

    sizes = jnp.where(number % 4 == 0, named(packed, number // 4), named(ordinary, number - number // 4 - 1))
    mixed = jax.random.permutation(jax.random.fold_in(own, 3), amount)
    donor, receiver = mixed[0:amount // 2 * 2:2], mixed[1:amount // 2 * 2:2]
    slack = jnp.minimum(sizes[donor] - 1, bound - sizes[receiver]) // 2
    slack = jnp.where((donor == order[0]) | (receiver == order[0]) | (sizes[receiver] == 0), 0, jnp.maximum(slack, 0))
    shifted = jax.random.randint(jax.random.fold_in(own, 4), (amount // 2,), 0, 1 << 20) % (slack + 1)
    sizes = sizes.at[donor].add(-shifted).at[receiver].add(shifted)
    labels = jnp.searchsorted(jnp.cumsum(sizes), jnp.arange(rows * top), side="right").astype(jnp.int32)
    table = labels.reshape(top, rows).T
    table = table[jax.random.permutation(jax.random.fold_in(own, 1), rows)]
    offset_by = jax.random.randint(jax.random.fold_in(own, 2), (rows, 1), 0, top)
    return jnp.take_along_axis(table, (jnp.arange(top)[None, :] + offset_by) % top, axis=1)


def load_shares(amount, total, reach, skew, full):
    portions = [(1 << 20) // math.isqrt(grade ** skew) + 1 for grade in range(1, amount + 1)]
    largest = reach if full else min(reach, max(-(-total // amount), total * portions[0] // sum(portions)))
    least = 1 if total - largest >= amount - 1 else 0
    counts, spare = [largest] + [least] * (amount - 1), total - largest - least * (amount - 1)
    while spare > 0:
        candidates = [i for i in range(1, amount) if counts[i] < largest] or [i for i in range(1, amount) if counts[i] < reach]
        whole, left = sum([portions[i] for i in candidates]), spare
        for i in candidates:
            more = min(reach - counts[i], max(1, left * portions[i] // whole), spare)
            counts[i] = counts[i] + more
            spare = spare - more
    return np.array(counts)


def noise(stream_key, shape, scale, most, cuts=(), kind=jnp.bfloat16):
    values = jax.random.normal(stream_key, shape, jnp.float32) * scale
    if len(cuts) > 0:
        values = levels(stream_key, shape, cuts, -0.22, 0.18) * values
    return jnp.clip(values, min=-most, max=most).astype(kind)


def setup_inputs(seed: int = 0, part: int = 0) -> dict:
    splits = jax.random.split(jax.random.key(seed), 13)
    own_keys = jax.random.split(jax.random.fold_in(splits[12], part), 13)
    a_tokens = noise(own_keys[0], (TA, D), 1.0, 6.0, ((0, 16),))
    a_gain = jnp.clip(1.0 + 0.15 * jax.random.normal(splits[1], (D,), jnp.float32), 0.25, 1.75)
    dense_gate = noise(splits[2], (D, FF), D ** -0.5, 0.0625, ((1, 16),))
    dense_up = noise(splits[3], (D, FF), D ** -0.5, 0.0625, ((1, 16),))
    dense_down = noise(splits[4], (FF, D), FF ** -0.5, 0.046875, ((0, 16),))
    b_tokens = noise(own_keys[5], (TB, D), 1.0, 6.0, ((0, 16),))
    b_gain = jnp.clip(1.0 + 0.15 * jax.random.normal(splits[6], (D,), jnp.float32), 0.25, 1.75)
    expert_ids_keys = jax.random.split(jax.random.fold_in(own_keys[7], 1), TB // TB_DEV)
    expert_ids_turns = jax.random.permutation(jax.random.fold_in(own_keys[7], 3), TB // TB_DEV)
    expert_ids = jax.vmap(lambda own, number: shared_out(jax.random.fold_in(own_keys[7], 2), own, number, TB_DEV, EXPERTS, TOPK, CAP, 2))(expert_ids_keys, expert_ids_turns).reshape((TB, TOPK))
    route_weights = jnp.clip(jnp.exp(math.log(0.5) - 2.3025851 * jax.random.uniform(own_keys[8], (TB, TOPK), jnp.float32) ** levels(own_keys[8], (TB, TOPK), ((0, 16),), -0.2, 0.2)), 0.05, 0.5)
    expert_gate = noise(splits[9], (EXPERTS * GROUP, D, ES), D ** -0.5, 0.0625, ((0, 16),))
    expert_up = noise(splits[10], (EXPERTS * GROUP, D, ES), D ** -0.5, 0.0625, ((0, 16),))
    expert_down = noise(splits[11], (EXPERTS * GROUP, ES, D), EH ** -0.5, 0.1875, ((0, 16),))
    return dict(a_tokens=a_tokens, a_gain=a_gain, dense_gate=dense_gate, dense_up=dense_up, dense_down=dense_down, b_tokens=b_tokens, b_gain=b_gain, expert_ids=expert_ids, route_weights=route_weights, expert_gate=expert_gate, expert_up=expert_up, expert_down=expert_down)


def normed(values, gain_vec):
    return values * lax.rsqrt(lax.optimization_barrier(jnp.mean(values * values, axis=-1, keepdims=True)) + 1e-06) * gain_vec

def reference(a_tokens, a_gain, dense_gate, dense_up, dense_down, b_tokens, b_gain, expert_ids, route_weights, expert_gate, expert_up, expert_down):
    a_float = a_tokens.astype(jnp.float32)
    a_normed = normed(a_float, a_gain).astype(jnp.bfloat16)
    gate_proj = jnp.dot(a_normed, dense_gate, preferred_element_type=jnp.float32)
    up_proj = jnp.dot(a_normed, dense_up, preferred_element_type=jnp.float32)
    hidden = (jax.nn.silu(gate_proj) * up_proj).astype(jnp.bfloat16)
    a_out = (a_float + jnp.dot(hidden, dense_down, preferred_element_type=jnp.float32)).astype(jnp.bfloat16)
    b_float = b_tokens.astype(jnp.float32)
    b_normed = normed(b_float, b_gain).astype(jnp.bfloat16)
    b_wide = b_normed.astype(jnp.float32)
    onehot = (expert_ids[:, :, None] == jnp.arange(EXPERTS, dtype=jnp.int32)[None, None, :]).astype(jnp.float32)
    mix_table = jnp.einsum('tk,tke->et', route_weights.astype(jnp.float32), onehot)
    gate_blocks = expert_gate.reshape(EXPERTS, GROUP, D, ES)
    up_blocks = expert_up.reshape(EXPERTS, GROUP, D, ES)
    down_blocks = expert_down.reshape(EXPERTS, GROUP, ES, D)

    def one_expert(running, inputs):
        w_gate, w_up, w_down, weight = inputs
        gate_e = jnp.einsum('td,gds->tgs', b_wide, w_gate.astype(jnp.float32))
        up_e = jnp.einsum('td,gds->tgs', b_wide, w_up.astype(jnp.float32))
        hid_e = (jax.nn.silu(gate_e) * up_e).astype(jnp.bfloat16)
        partial_value = jnp.einsum('tgs,gsd->tgd', hid_e.astype(jnp.float32), w_down.astype(jnp.float32)).astype(jnp.bfloat16)
        expert_out = lax.optimization_barrier(jnp.sum(partial_value.astype(jnp.float32), axis=1)).astype(jnp.bfloat16)
        return (running + weight[:, None] * expert_out.astype(jnp.float32), None)
    totals, _ = lax.scan(one_expert, jnp.zeros((TB, D), jnp.float32), (gate_blocks, up_blocks, down_blocks, mix_table))
    b_out = (b_float + totals).astype(jnp.bfloat16)
    return (a_out, b_out)
```

```python
import functools

import jax
import jax.numpy as jnp
from jax import lax
from jax.experimental import pallas as pl
from jax.experimental.pallas import tpu as pltpu
from jax.sharding import PartitionSpec as P

EXPERTS = 16
LANES = 128
EARLY = 6
LAG = 2
F32 = jnp.float32
BF16 = jnp.bfloat16


def pick(total, sizes):
    for size in sizes:
        if total % size == 0:
            return size
    return total


def normed(values, gain_row):
    mean = jnp.mean(values * values, axis=-1, keepdims=True)
    return values * lax.rsqrt(mean + 1e-06) * gain_row


def kernel(
    n, kc, cn,
    a_ref, ag_ref, b_ref, bg_ref, ids_ref, rw_ref,
    dg_hbm, du_hbm, dd_hbm, eg_hbm, eu_hbm, ed_hbm,
    a_out, b_out,
    gu, dn, gat_b, gat_a, g_acc, u_acc, hid_b, hid_a,
    mine_b, s1_b, r1_b, s2_b, r2_b,
    mine_a, s1_a, r1_a, s2_a, r2_a,
    gu_sem, dn_sem, gat_send, gat_recv, fwd_send, fwd_recv,
    s1_send, s1_recv, s2_send, s2_recv,
):
    me = lax.axis_index("exp")
    core = lax.rem(me, 2)
    chip = me // 2
    chips = n // 2
    sibling = chip * 2 + (1 - core)
    expert = me // (n // EXPERTS)
    width = a_ref.shape[1]
    steps = width // kc
    groups = width // cn
    es = eg_hbm.shape[2]
    fd = dg_hbm.shape[1]
    wide = gu.shape[3]
    tall = dn.shape[1]

    def peer(offset):
        return lax.rem(chip + offset + chips, chips) * 2 + core

    def cols(j, size):
        return pl.ds(pl.multiple_of(j * size, size), size)

    def slot_gu(which, k, used):
        return gu.at[which, k] if used == wide else gu.at[which, k, :, pl.ds(0, used)]

    def slot_dn(j, used):
        return dn.at[j] if used == tall else dn.at[j, pl.ds(0, used), :]

    def e_gu(which, k):
        src = (eg_hbm, eu_hbm)[which].at[0, cols(k, kc), :]
        return pltpu.make_async_copy(src, slot_gu(which, k, es), gu_sem.at[which, k])

    def d_gu(which, k):
        src = (dg_hbm, du_hbm)[which].at[cols(k, kc), :]
        return pltpu.make_async_copy(src, slot_gu(which, k, fd), gu_sem.at[which, k])

    def e_dn(j):
        return pltpu.make_async_copy(ed_hbm.at[0, :, cols(j, cn)], slot_dn(j, es), dn_sem.at[j])

    def d_dn(j):
        return pltpu.make_async_copy(dd_hbm.at[:, cols(j, cn)], slot_dn(j, fd), dn_sem.at[j])

    def start_gu(k, carry):
        e_gu(0, k).start()
        e_gu(1, k).start()
        return carry

    def start_dn(j, carry):
        e_dn(j).start()
        return carry

    barrier = pltpu.get_barrier_semaphore()

    def greet(o, carry):
        pl.semaphore_signal(
            barrier, inc=1, device_id={"exp": peer(o)}, device_id_type=pl.DeviceIdType.MESH
        )
        return carry

    lax.fori_loop(1, chips, greet, 0)
    pl.semaphore_signal(
        barrier, inc=1, device_id={"exp": sibling}, device_id_type=pl.DeviceIdType.MESH
    )
    early = min(EARLY, steps)
    lax.fori_loop(0, early, start_gu, 0)

    rows_b = b_ref.shape[0]
    gat_b[0, core, :, pl.ds(0, width)] = normed(b_ref[...].astype(F32), bg_ref[...]).astype(BF16)
    lane = lax.broadcasted_iota(jnp.int32, (rows_b, LANES), 1)
    table = jnp.zeros((rows_b, LANES), F32)
    for k in range(ids_ref.shape[1]):
        table = table + jnp.where(ids_ref[:, k : k + 1] == lane, rw_ref[:, k : k + 1], 0.0)
    high = table.astype(BF16)
    gat_b[0, core, :, pl.ds(width, LANES)] = high
    gat_b[0, core, :, pl.ds(width + LANES, LANES)] = (table - high.astype(F32)).astype(BF16)
    gat_a[0, core] = normed(a_ref[...].astype(F32), ag_ref[...]).astype(BF16)

    pl.semaphore_wait(barrier, chips)

    def remote(src, dst, send, recv, target):
        return pltpu.make_async_remote_copy(
            src_ref=src, dst_ref=dst, send_sem=send, recv_sem=recv,
            device_id={"exp": target}, device_id_type=pl.DeviceIdType.MESH,
        )

    def gather_copy(ph, o):
        buf = (gat_b, gat_a)[ph]
        return remote(
            buf.at[0, core], buf.at[o, core], gat_send.at[ph], gat_recv.at[ph, o], peer(o)
        )

    def forward_copy(ph, o):
        buf = (gat_b, gat_a)[ph]
        return remote(
            buf.at[o, core], buf.at[o, core], fwd_send.at[ph], fwd_recv.at[ph], sibling
        )

    def gather_start(ph):
        def go(o, carry):
            gather_copy(ph, o).start()
            return carry

        lax.fori_loop(1, chips, go, 0)
        forward_copy(ph, 0).start()

    def gather_forward(ph):
        def go(o, carry):
            gather_copy(ph, o).wait_recv()
            forward_copy(ph, o).start()
            return carry

        lax.fori_loop(1, chips, go, 0)

    def gather_finish(ph):
        buf = (gat_b, gat_a)[ph]
        block = buf.at[:, 1 - core]
        pltpu.make_async_copy(block, block, fwd_recv.at[ph]).wait()

    gather_start(0)
    gather_start(1)
    lax.fori_loop(early, steps, start_gu, 0)
    lax.fori_loop(0, groups, start_dn, 0)
    gather_forward(0)
    gather_finish(0)

    def rows_of(buf, where):
        pieces = [buf[o, c, :, where].astype(F32) for c in range(2) for o in range(chips)]
        return jnp.concatenate(pieces, axis=0)

    def hidden(ph, used, copy, after, buf, out):
        total = buf.shape[0] * 2 * buf.shape[2]
        ga = g_acc.at[pl.ds(0, total), pl.ds(0, used)]
        ua = u_acc.at[pl.ds(0, total), pl.ds(0, used)]
        ga[...] = jnp.zeros(ga.shape, F32)
        ua[...] = jnp.zeros(ua.shape, F32)

        def step(k, carry):
            x = rows_of(buf, cols(k, kc)).astype(BF16)
            copy(0, k).wait()
            ga[...] += jnp.dot(x, slot_gu(0, k, used)[...], preferred_element_type=F32)
            copy(1, k).wait()
            ua[...] += jnp.dot(x, slot_gu(1, k, used)[...], preferred_element_type=F32)
            after(k)
            return carry

        lax.fori_loop(0, steps, step, 0)
        g = ga[...]
        out[...] = (g / (1.0 + jnp.exp(-g)) * ua[...]).astype(BF16)

    def pair_copy(ph, j):
        src, dst = ((s1_b, r1_b), (s1_a, r1_a))[ph]
        return remote(
            src.at[:, cols(j, cn)], dst.at[:, cols(j, cn)],
            s1_send.at[ph], s1_recv.at[ph, j], sibling,
        )

    def down(ph, used, copy, after, hid, scale):
        mine, s1, r1, s2, r2 = (
            (mine_b, s1_b, r1_b, s2_b, r2_b), (mine_a, s1_a, r1_a, s2_a, r2_a)
        )[ph]
        half = mine.shape[0]
        rows = half // chips

        def finish(j):
            where = cols(j, cn)
            pair_copy(ph, j).wait_recv()
            both = mine[:, where] + r1[:, where].astype(F32)
            mine[:, where] = both
            for o in range(1, chips):
                s2[o - 1, :, where] = both[o * rows : (o + 1) * rows].astype(BF16)

            def send(o, carry):
                remote(
                    s2.at[o - 1, :, where], r2.at[o - 1, :, where],
                    s2_send.at[ph], s2_recv.at[ph], peer(-o),
                ).start()
                return carry

            lax.fori_loop(1, chips, send, 0)

        def step(j, carry):
            where = cols(j, cn)
            copy(j).wait()
            part = jnp.dot(hid[...], slot_dn(j, used)[...], preferred_element_type=F32)
            if scale is not None:
                part = part * scale
            first, second = part[:half], part[half:]
            mine[:, where] = jnp.where(core == 0, first, second)
            s1[:, where] = jnp.where(core == 0, second, first).astype(BF16)
            pair_copy(ph, j).start()
            after(j)

            @pl.when(j >= LAG)
            def _():
                finish(j - LAG)

            return carry

        lax.fori_loop(0, groups, step, 0)

        def rest(j, carry):
            finish(j)
            return carry

        lax.fori_loop(max(groups - LAG, 0), groups, rest, 0)

    def result(ph, own, out):
        mine, r2 = ((mine_b, r2_b), (mine_a, r2_a))[ph]
        pltpu.make_async_copy(r2, r2, s2_recv.at[ph]).wait()
        rows = out.shape[0]

        def step(j, carry):
            where = cols(j, cn)
            total = mine[pl.ds(0, rows), where]
            for o in range(chips - 1):
                total = total + r2[o, :, where].astype(F32)
            out[:, where] = (own[:, where].astype(F32) + total).astype(BF16)
            return carry

        lax.fori_loop(0, groups, step, 0)

    def next_gu(k):
        d_gu(0, k).start()
        d_gu(1, k).start()

    def nothing(k):
        return None

    hidden(0, es, e_gu, next_gu, gat_b, hid_b)
    gather_forward(1)
    tables = rows_of(gat_b, pl.ds(width, LANES)) + rows_of(gat_b, pl.ds(width + LANES, LANES))
    chosen = lax.broadcasted_iota(jnp.int32, tables.shape, 1) == expert
    scale = jnp.sum(jnp.where(chosen, tables, 0.0), axis=1, keepdims=True)
    down(0, es, e_dn, lambda j: d_dn(j).start(), hid_b, scale)
    gather_finish(1)
    hidden(1, fd, d_gu, nothing, gat_a, hid_a)
    down(1, fd, d_dn, nothing, hid_a, None)
    result(0, b_ref, b_out)
    result(1, a_ref, a_out)

    for ph in range(2):
        buf = (gat_b, gat_a)[ph]
        s1, s2 = ((s1_b, s2_b), (s1_a, s2_a))[ph]
        sent = buf.at[pl.ds(0, chips - 1), 0]
        pltpu.make_async_copy(sent, sent, gat_send.at[ph]).wait()
        sent = buf.at[:, 0]
        pltpu.make_async_copy(sent, sent, fwd_send.at[ph]).wait()
        pltpu.make_async_copy(s1, s1, s1_send.at[ph]).wait()
        pltpu.make_async_copy(s2, s2, s2_send.at[ph]).wait()


def shards(
    a_tokens, a_gain, dense_gate, dense_up, dense_down, b_tokens, b_gain, expert_ids,
    route_weights, expert_gate, expert_up, expert_down,
):
    n = lax.axis_size("exp")
    chips = n // 2
    ra, width = a_tokens.shape
    rb = b_tokens.shape[0]
    fd = dense_gate.shape[1]
    es = expert_gate.shape[2]
    wide = max(fd, es)
    kc = pick(width, (512, 256, 128))
    cn = pick(width, (1024, 512, 256, 128))
    steps, groups = width // kc, width // cn
    extra = width + 2 * LANES
    most = n * max(ra, rb)

    def back(rows):
        return [
            pltpu.VMEM((chips * rows, width), F32),
            pltpu.VMEM((chips * rows, width), BF16),
            pltpu.VMEM((chips * rows, width), BF16),
            pltpu.VMEM((chips - 1, rows, width), BF16),
            pltpu.VMEM((chips - 1, rows, width), BF16),
        ]

    vmem = pl.BlockSpec(memory_space=pltpu.VMEM)
    hbm = pl.BlockSpec(memory_space=pl.ANY)
    dma = pltpu.SemaphoreType.DMA
    weights = 3 * width * (fd + es)
    return pl.pallas_call(
        functools.partial(kernel, n, kc, cn),
        out_shape=(
            jax.ShapeDtypeStruct(a_tokens.shape, BF16),
            jax.ShapeDtypeStruct(b_tokens.shape, BF16),
        ),
        in_specs=[vmem] * 6 + [hbm] * 6,
        out_specs=(vmem, vmem),
        scratch_shapes=[
            pltpu.VMEM((2, steps, kc, wide), BF16),
            pltpu.VMEM((groups, wide, cn), BF16),
            pltpu.VMEM((chips, 2, rb, extra), BF16),
            pltpu.VMEM((chips, 2, ra, width), BF16),
            pltpu.VMEM((most, wide), F32),
            pltpu.VMEM((most, wide), F32),
            pltpu.VMEM((n * rb, es), BF16),
            pltpu.VMEM((n * ra, fd), BF16),
            *back(rb),
            *back(ra),
            dma((2, steps)),
            dma((groups,)),
            dma((2,)),
            dma((2, chips)),
            dma((2,)),
            dma((2,)),
            dma((2,)),
            dma((2, groups)),
            dma((2,)),
            dma((2,)),
        ],
        compiler_params=pltpu.CompilerParams(
            collective_id=0, has_side_effects=True, vmem_limit_bytes=67043328
        ),
        cost_estimate=pl.CostEstimate(
            flops=2 * n * max(ra, rb) * weights, bytes_accessed=2 * weights, transcendentals=0
        ),
    )(
        a_tokens, a_gain.reshape(1, width), b_tokens, b_gain.reshape(1, width),
        expert_ids, route_weights,
        dense_gate, dense_up, dense_down, expert_gate, expert_up, expert_down,
    )


def solution(mesh):
    return jax.shard_map(
        shards,
        mesh=mesh,
        in_specs=(
            P(("rep", "exp"), None),
            P(),
            P(None, "exp"),
            P(None, "exp"),
            P("exp", None),
            P(("rep", "exp"), None),
            P(),
            P(("rep", "exp"), None),
            P(("rep", "exp"), None),
            P("exp", None, None),
            P("exp", None, None),
            P("exp", None, None),
        ),
        out_specs=(P(("rep", "exp"), None), P(("rep", "exp"), None)),
        check_vma=False,
    )
```
